64 devices in a mesh: graph: 4 (over x, y), nodes: 16 (over z, core).
Axes of the slice: x: 2, y: 2, z: 8, core: 2. Of those that a mesh axis runs over, the one named last changes fastest.
The devices are a block of a 4x4x8 slice.
Arguments:
- node_feats: bfloat16 [98304, 1433], P(('graph', 'nodes')), parts along dimension 0
- a_int: bfloat16 [98304, 1536], P(('graph', 'nodes')), parts along dimension 0
- a_halo: bfloat16 [98304, 512], P(('graph', 'nodes')), parts along dimension 0
- send_idx: int32 [256, 128], P(('graph', 'nodes')), parts along dimension 0
- w_first: bfloat16 [1433, 16], replicated
- w_second: bfloat16 [16, 7], replicated
- grad_out: bfloat16 [98304, 7], P(('graph', 'nodes')), parts along dimension 0
Outputs:
- output 1: float32 [5732, 16], P('graph'), parts along dimension 0
- output 2: float32 [64, 7], P('graph'), parts along dimension 0
- output 3: float32 [98304, 1433], P(('graph', 'nodes')), parts along dimension 0
There are 4 independent parts. The reference program is written for one: setup_inputs(seed, part) draws one part's arguments, and reference() takes and returns one part's arrays. A program takes and returns all parts, laid end to end along the dimension named above; an argument that names none is the same for every part.
All inputs are finite; a program needn't handle non-finite values.
Results may differ from the reference program's by a relative error of at most 0.00548394.
Values are sent between devices in bfloat16 or wider.
A program may use at most 768 MiB of HBM per device.

```python
import jax
import jax.numpy as jnp
from jax import lax

GROUP_SIZE = 16
NODES_DEV = 1536
HALO_SLOTS = 128
MAX_HOPS = 2
FEAT_IN = 1433
HIDDEN = 16
CLASSES = 7
INNER_DEGREE = 16
HALO_DEGREE = 4

NUM_LINKS = 2 * MAX_HOPS
OFFSETS = [(link // 2 + 1) * (1 - 2 * (link % 2)) for link in range(NUM_LINKS)]


def draw_graph(key):
    key_count, key_order, key_blocks = jax.random.split(key, 3)
    window = 2 * HALO_SLOTS
    counts = jax.random.randint(key_count, (GROUP_SIZE, NUM_LINKS), HALO_SLOTS // 4, HALO_SLOTS + 1)
    counts = counts.at[0, 0].set(HALO_SLOTS)
    scores = jax.random.randint(key_order, (GROUP_SIZE, NUM_LINKS, window), 0, 65536) * window + jnp.arange(window)
    slot_order = jnp.argsort(scores, axis=-1)[:, :, :HALO_SLOTS]
    upward = jnp.array([offset > 0 for offset in OFFSETS])
    window_base = jnp.where(upward, NODES_DEV - window, 0)
    slot_pos = jnp.arange(HALO_SLOTS)
    used_slot = slot_pos[None, None, :] < counts[:, :, None]
    send_idx = jnp.where(used_slot, slot_order + window_base[None, :, None], 0).astype(jnp.int32)
    recv_counts = jnp.stack([jnp.roll(counts[:, link], OFFSETS[link]) for link in range(NUM_LINKS)], axis=1)
    row_pos = jnp.arange(NODES_DEV)
    low_half = row_pos < NODES_DEV // 2
    row_ok = jnp.where(upward[None, :], low_half[:, None], jnp.logical_not(low_half)[:, None])

    def one_device(inputs):
        dev_key, recv_count = inputs
        key_mask, key_inner, key_hmask, key_halo = jax.random.split(dev_key, 4)
        inner_mask = jnp.logical_or(jax.random.randint(key_mask, (NODES_DEV, NODES_DEV), 0, NODES_DEV) < INNER_DEGREE, row_pos[:, None] == row_pos[None, :])
        col_ok = slot_pos[None, :] < recv_count[:, None]
        halo_mask = (jax.random.randint(key_hmask, (NODES_DEV, NUM_LINKS, HALO_SLOTS), 0, HALO_SLOTS) < HALO_DEGREE) & row_ok[:, :, None] & col_ok[None, :, :]
        inner_w = jnp.where(inner_mask, jax.random.uniform(key_inner, (NODES_DEV, NODES_DEV), jnp.float32, 0.5, 1.5), 0.0)
        halo_w = jnp.where(halo_mask, jax.random.uniform(key_halo, (NODES_DEV, NUM_LINKS, HALO_SLOTS), jnp.float32, 0.5, 1.5), 0.0)
        degree = jnp.sum(inner_mask, axis=1) + jnp.sum(halo_mask, axis=(1, 2))
        row_scale = lax.rsqrt(degree.astype(jnp.float32))
        inner_adj = (inner_w * row_scale[:, None]).astype(jnp.bfloat16)
        halo_adj = (halo_w * row_scale[:, None, None]).reshape(NODES_DEV, NUM_LINKS * HALO_SLOTS).astype(jnp.bfloat16)
        return inner_adj, halo_adj

    inner_adj, halo_adj = lax.map(one_device, (jax.random.split(key_blocks, GROUP_SIZE), recv_counts))
    return (inner_adj.reshape(GROUP_SIZE * NODES_DEV, NODES_DEV), halo_adj.reshape(GROUP_SIZE * NODES_DEV, NUM_LINKS * HALO_SLOTS), send_idx.reshape(GROUP_SIZE * NUM_LINKS, HALO_SLOTS))


def setup_inputs(seed: int = 0, part: int = 0) -> dict:
    root_key = jax.random.key(seed)
    shared_key, parts_key = jax.random.split(root_key)
    key_first, key_second = jax.random.split(shared_key)
    part_key = jax.random.fold_in(parts_key, part)
    key_feats, key_grad, key_graph = jax.random.split(part_key, 3)
    rows_total = GROUP_SIZE * NODES_DEV
    node_feats = jax.random.normal(key_feats, (rows_total, FEAT_IN), jnp.float32).astype(jnp.bfloat16)
    grad_out = jax.random.normal(key_grad, (rows_total, CLASSES), jnp.float32).astype(jnp.bfloat16)
    w_first = (jax.random.normal(key_first, (FEAT_IN, HIDDEN), jnp.float32) * FEAT_IN ** -0.5).astype(jnp.bfloat16)
    w_second = (jax.random.normal(key_second, (HIDDEN, CLASSES), jnp.float32) * HIDDEN ** -0.5).astype(jnp.bfloat16)
    a_int, a_halo, send_idx = draw_graph(key_graph)
    return {"node_feats": node_feats, "a_int": a_int, "a_halo": a_halo, "send_idx": send_idx, "w_first": w_first, "w_second": w_second, "grad_out": grad_out}


def aggregate(a_int, a_halo, features, send_idx):
    feat_width = features.shape[-1]
    local_rows = features.reshape(GROUP_SIZE, NODES_DEV, feat_width)
    send_plan = send_idx.reshape(GROUP_SIZE, NUM_LINKS * HALO_SLOTS)
    sent_rows = jax.vmap(lambda rows_dev, plan_dev: jnp.take(rows_dev, plan_dev, axis=0))(local_rows, send_plan)
    sent_rows = sent_rows.reshape(GROUP_SIZE, NUM_LINKS, HALO_SLOTS, feat_width)
    halo_rows = jnp.stack([jnp.roll(sent_rows[:, link], OFFSETS[link], axis=0) for link in range(NUM_LINKS)], axis=1)
    halo_rows = halo_rows.reshape(GROUP_SIZE, NUM_LINKS * HALO_SLOTS, feat_width)
    blocks = (a_int.reshape(GROUP_SIZE, NODES_DEV, NODES_DEV), a_halo.reshape(GROUP_SIZE, NODES_DEV, NUM_LINKS * HALO_SLOTS), local_rows, halo_rows)

    def one_device(block):
        inner_adj, halo_adj, own_rows, remote_rows = block
        return jnp.dot(inner_adj, own_rows, preferred_element_type=jnp.float32) + jnp.dot(halo_adj, remote_rows, preferred_element_type=jnp.float32)

    return lax.map(one_device, blocks).reshape(GROUP_SIZE * NODES_DEV, feat_width)


def aggregate_back(a_int, a_halo, grad_rows, send_idx):
    feat_width = grad_rows.shape[-1]
    local_rows = grad_rows.reshape(GROUP_SIZE, NODES_DEV, feat_width)
    blocks = (a_int.reshape(GROUP_SIZE, NODES_DEV, NODES_DEV), a_halo.reshape(GROUP_SIZE, NODES_DEV, NUM_LINKS * HALO_SLOTS), local_rows)

    def one_device(block):
        inner_adj, halo_adj, own_rows = block
        inner_sum = jnp.dot(inner_adj.T, own_rows, preferred_element_type=jnp.float32)
        outward = jnp.dot(halo_adj.T, own_rows, preferred_element_type=jnp.float32).astype(jnp.bfloat16)
        return inner_sum, outward

    inner_sum, outward = lax.map(one_device, blocks)
    outward = outward.reshape(GROUP_SIZE, NUM_LINKS, HALO_SLOTS, feat_width)
    returned = jnp.stack([jnp.roll(outward[:, link], -OFFSETS[link], axis=0) for link in range(NUM_LINKS)], axis=1)
    returned = returned.reshape(GROUP_SIZE, NUM_LINKS * HALO_SLOTS, feat_width)
    send_plan = send_idx.reshape(GROUP_SIZE, NUM_LINKS * HALO_SLOTS)
    total_sum = jax.vmap(lambda sums_dev, plan_dev, rows_dev: sums_dev.at[plan_dev].add(rows_dev.astype(jnp.float32)))(inner_sum, send_plan, returned)
    return total_sum.reshape(GROUP_SIZE * NODES_DEV, feat_width)


def reference(node_feats, a_int, a_halo, send_idx, w_first, w_second, grad_out):
    z_first = aggregate(a_int, a_halo, node_feats, send_idx).astype(jnp.bfloat16)
    hidden = jnp.maximum(jnp.dot(z_first, w_first, preferred_element_type=jnp.float32), 0.0).astype(jnp.bfloat16)
    z_second = aggregate(a_int, a_halo, hidden, send_idx).astype(jnp.bfloat16)
    dw_second = jnp.dot(z_second.T, grad_out, preferred_element_type=jnp.float32)
    dz_second = jnp.dot(grad_out, w_second.T, preferred_element_type=jnp.float32).astype(jnp.bfloat16)
    d_hidden = aggregate_back(a_int, a_halo, dz_second, send_idx)
    grad_pre = jnp.where(hidden > 0, d_hidden, 0.0).astype(jnp.bfloat16)
    dw_first = jnp.dot(z_first.T, grad_pre, preferred_element_type=jnp.float32)
    dz_first = jnp.dot(grad_pre, w_first.T, preferred_element_type=jnp.float32).astype(jnp.bfloat16)
    grad_feats = aggregate_back(a_int, a_halo, dz_first, send_idx)
    return (dw_first, dw_second, grad_feats)
```

```python
import functools

import jax
import jax.numpy as jnp
from jax import lax
from jax.experimental import pallas as pl
from jax.experimental.pallas import tpu as pltpu
from jax.sharding import PartitionSpec as P

MESH = pl.DeviceIdType.MESH
BF16 = jnp.bfloat16
F32 = jnp.float32
ROWS = 256
LANES = 128


def link_offsets(num_links):
    return [(link // 2 + 1) * (1 - 2 * (link % 2)) for link in range(num_links)]


def nn(left, right):
    return lax.dot_general(left, right, (((1,), (0,)), ((), ())), preferred_element_type=F32)


def nt(left, right):
    return lax.dot_general(left, right, (((1,), (1,)), ((), ())), preferred_element_type=F32)


def tn(left, right):
    return lax.dot_general(left, right, (((0,), (0,)), ((), ())), preferred_element_type=F32)


def halves(value):
    high = value.astype(BF16)
    return high, (value - high.astype(F32)).astype(BF16)


def chunks_of(total, size):
    return [(start, min(size, total - start)) for start in range(0, total, size)]


def round_up(value, multiple):
    return -(-value // multiple) * multiple


def graph_kernel(n, x_hbm, a_hbm, ah_hbm, idx_ref, w1_ref, w2_ref, g_ref,
                 t_ref, dw_ref,
                 x, a, ah, hot, send, recv, acc, z, g_send, g_recv, f_send, f_recv, part, part_in, total,
                 x_sem, a_sem, ah_sem, s_sem, r_sem, gs_sem, gr_sem, fs_sem, fr_sem, ps_sem, pr_sem, ts_sem, tr_sem):
    feats, nodes = x_hbm.shape
    num_links = idx_ref.shape[0]
    slots = idx_ref.shape[1]
    hidden = w1_ref.shape[0]
    classes = w2_ref.shape[0]
    offsets = link_offsets(num_links)
    steps = chunks_of(feats, ROWS)
    me = lax.axis_index("nodes")

    def peer(offset):
        return {"nodes": lax.rem(me + offset + n, n)}

    x_copies = [pltpu.make_async_copy(x_hbm.at[pl.ds(start, size)], x.at[pl.ds(start, size)], x_sem.at[c]) for c, (start, size) in enumerate(steps)]
    a_copy = pltpu.make_async_copy(a_hbm, a, a_sem)
    ah_copy = pltpu.make_async_copy(ah_hbm, ah, ah_sem)
    for copy in x_copies:
        copy.start()
    ah_copy.start()
    a_copy.start()

    barrier = pltpu.get_barrier_semaphore()
    for far in range(1, n):
        pl.semaphore_signal(barrier, inc=1, device_id=peer(far), device_id_type=MESH)

    row_pos = lax.broadcasted_iota(jnp.int32, (nodes, slots), 0)
    for link in range(num_links):
        hot[:, link * slots:(link + 1) * slots] = jnp.where(row_pos == idx_ref[link:link + 1, :], 1.0, 0.0).astype(BF16)

    pl.semaphore_wait(barrier, n - 1)

    x_sends = []
    for c, (start, size) in enumerate(steps):
        x_copies[c].wait()
        send[start:start + size, :] = nn(x[start:start + size, :], hot[...]).astype(BF16)
        for link, offset in enumerate(offsets):
            where = (pl.ds(start, size), pl.ds(link * slots, slots))
            copy = pltpu.make_async_remote_copy(send.at[where], recv.at[where], s_sem.at[c, link], r_sem.at[c, link], device_id=peer(offset), device_id_type=MESH)
            copy.start()
            x_sends.append(copy)

    def send_back(source, target, source_sem, target_sem):
        copies = []
        for link, offset in enumerate(offsets):
            where = (slice(None), pl.ds(link * slots, slots))
            copy = pltpu.make_async_remote_copy(source.at[where], target.at[where], source_sem.at[link], target_sem.at[link], device_id=peer(-offset), device_id_type=MESH)
            copy.start()
            copies.append(copy)
        return copies

    g_rows = g_ref[...]
    e_rows = tn(w2_ref[...], g_rows).astype(BF16)
    eg = jnp.concatenate([e_rows, g_rows, jnp.zeros((16 - classes, nodes), BF16)], axis=0)
    ah_copy.wait()
    outward = nn(eg, ah[...])
    g_send[...] = jnp.concatenate([outward[:hidden].astype(BF16).astype(F32), outward[hidden:hidden + 8]], axis=0)
    g_sends = send_back(g_send, g_recv, gs_sem, gr_sem)

    a_copy.wait()
    eg_sum = nn(eg, a[...])

    for c, (start, size) in enumerate(steps):
        acc[start:start + size, :] = nt(x[start:start + size, :], a[...])

    for copy in g_sends:
        copy.wait()
    g_high, g_low = halves(g_recv[hidden:, :])
    back = nt(jnp.concatenate([g_recv[:hidden, :].astype(BF16), g_high, g_low], axis=0), hot[...])
    d_rows = eg_sum[:hidden] + back[:hidden]
    u_rows = eg_sum[hidden:hidden + 8] + back[hidden:hidden + 8] + back[hidden + 8:hidden + 16]
    u_high, u_low = halves(u_rows)

    pre = jnp.zeros((hidden, nodes), F32)
    for c, (start, size) in enumerate(steps):
        for link in range(num_links):
            x_sends[c * num_links + link].wait()
        z_rows = (acc[start:start + size, :] + nt(recv[start:start + size, :], ah[...])).astype(BF16)
        z[start:start + size, :] = z_rows
        pre = pre + nn(w1_ref[:, start:start + size], z_rows)

    h_rows = jnp.maximum(pre, 0.0).astype(BF16)
    f_rows = jnp.where(h_rows.astype(F32) > 0.0, d_rows, 0.0).astype(BF16)

    f_send[...] = nn(f_rows, ah[...])
    f_sends = send_back(f_send, f_recv, fs_sem, fr_sem)

    dw = nt(f_rows, z[...])
    dw2 = nt(h_rows, u_high) + nt(h_rows, u_low)
    wide = part.shape[2]
    edge = wide - LANES
    for h in range(hidden):
        part[h, :, :feats] = dw[h:h + 1, :]
        part[h, :, edge:edge + 8] = dw2[h:h + 1, :]
    p_sends = []
    for far in range(1, n):
        to = lax.rem(me + far, n)
        copy = pltpu.make_async_remote_copy(part.at[to], part_in.at[far], ps_sem.at[far], pr_sem.at[far], device_id=peer(far), device_id_type=MESH)
        copy.start()
        p_sends.append(copy)

    t_rows = nn(f_rows, a[...])
    for copy in f_sends:
        copy.wait()
    f_high, f_low = halves(f_recv[...])
    f_back = nt(jnp.concatenate([f_high, f_low], axis=0), hot[...])
    t_rows = t_rows + f_back[:hidden] + f_back[hidden:]
    t_high, t_low = halves(t_rows)
    t_ref[...] = jnp.concatenate([t_high, t_low], axis=0)

    mine = part[me]
    for copy in p_sends:
        copy.wait()
    for far in range(1, n):
        mine = mine + part_in[far]
    total[me] = mine
    t_sends = []
    for far in range(1, n):
        copy = pltpu.make_async_remote_copy(total.at[me], total.at[me], ts_sem.at[far], tr_sem.at[far], device_id=peer(far), device_id_type=MESH)
        copy.start()
        t_sends.append(copy)
    for copy in t_sends:
        copy.wait()
    dw_ref[...] = total[...]


def grad_kernel(w1_ref, t_ref, dw_ref, out_ref, dw1_ref, dw2_ref):
    hidden, feats = dw1_ref.shape
    classes = dw2_ref.shape[0]
    w = w1_ref[...]
    out_ref[...] = tn(jnp.concatenate([w, w], axis=0), t_ref[...])

    @pl.when(pl.program_id(0) == 0)
    def _():
        edge = dw_ref.shape[2] - LANES
        for h in range(hidden):
            dw1_ref[h:h + 1, :] = dw_ref[h, :, :feats]
        tail = jnp.concatenate([dw_ref[h, :, edge:] for h in range(hidden)] + [jnp.zeros((LANES - hidden, LANES), F32)], axis=0)
        dw2_ref[...] = tail.T[:classes, :hidden]


def solution(mesh):
    n = mesh.shape["nodes"]
    row_spec = P(("graph", "nodes"), None)
    replicated = P(None, None)
    part_spec = P("graph", None)
    vmem = pl.BlockSpec(memory_space=pltpu.VMEM)
    hbm = pl.BlockSpec(memory_space=pl.ANY)

    def device_step(node_feats, a_int, a_halo, send_idx, w_first, w_second, grad_out):
        nodes, feats = node_feats.shape
        num_links, slots = send_idx.shape
        hidden, classes = w_second.shape
        assert hidden == n and classes <= 8
        halo = num_links * slots
        padded = round_up(feats, 16)
        wide = round_up(feats, LANES) + LANES
        num_steps = len(chunks_of(feats, ROWS))
        w1 = w_first.T
        dma = pltpu.SemaphoreType.DMA
        t_parts, dw = pl.pallas_call(
            functools.partial(graph_kernel, n),
            out_shape=(jax.ShapeDtypeStruct((2 * hidden, nodes), BF16), jax.ShapeDtypeStruct((hidden, 1, wide), F32)),
            in_specs=[hbm, hbm, hbm, vmem, vmem, vmem, vmem],
            out_specs=(vmem, vmem),
            scratch_shapes=[
                pltpu.VMEM((feats, nodes), BF16),
                pltpu.VMEM((nodes, nodes), BF16),
                pltpu.VMEM((nodes, halo), BF16),
                pltpu.VMEM((nodes, halo), BF16),
                pltpu.VMEM((feats, halo), BF16),
                pltpu.VMEM((feats, halo), BF16),
                pltpu.VMEM((feats, nodes), F32),
                pltpu.VMEM((feats, nodes), BF16),
                pltpu.VMEM((hidden + 8, halo), F32),
                pltpu.VMEM((hidden + 8, halo), F32),
                pltpu.VMEM((hidden, halo), F32),
                pltpu.VMEM((hidden, halo), F32),
                pltpu.VMEM((hidden, 1, wide), F32),
                pltpu.VMEM((n, 1, wide), F32),
                pltpu.VMEM((hidden, 1, wide), F32),
                dma((num_steps,)), dma, dma,
                dma((num_steps, num_links)), dma((num_steps, num_links)),
                dma((num_links,)), dma((num_links,)), dma((num_links,)), dma((num_links,)),
                dma((n,)), dma((n,)), dma((n,)), dma((n,)),
            ],
            compiler_params=pltpu.CompilerParams(collective_id=0, has_side_effects=True, vmem_limit_bytes=60 * 1024 * 1024),
            name="graph_kernel",
        )(node_feats.T, a_int, a_halo, send_idx, w1, w_second.T, grad_out.T)

        block = 256
        grads, dw1, dw2 = pl.pallas_call(
            grad_kernel,
            grid=(pl.cdiv(feats, block),),
            out_shape=(jax.ShapeDtypeStruct((feats, nodes), F32), jax.ShapeDtypeStruct((hidden, feats), F32), jax.ShapeDtypeStruct((classes, hidden), F32)),
            in_specs=[
                pl.BlockSpec((hidden, block), lambda i: (0, i)),
                pl.BlockSpec((2 * hidden, nodes), lambda i: (0, 0)),
                pl.BlockSpec((hidden, 1, wide), lambda i: (0, 0, 0)),
            ],
            out_specs=(
                pl.BlockSpec((block, nodes), lambda i: (i, 0)),
                pl.BlockSpec((hidden, feats), lambda i: (0, 0)),
                pl.BlockSpec((classes, hidden), lambda i: (0, 0)),
            ),
            name="grad_kernel",
        )(w1, t_parts, dw)
        return dw1.T, dw2.T, grads.T

    return jax.shard_map(device_step, mesh=mesh, in_specs=(row_spec, row_spec, row_spec, row_spec, replicated, replicated, row_spec), out_specs=(part_spec, part_spec, row_spec), check_vma=False)
```
